32 devices in a mesh: grp: 4 (over y, core), ep: 8 (over z, x).
Axes of the slice: x: 2, y: 2, z: 4, core: 2. Of those that a mesh axis runs over, the one named last changes fastest.
Arguments:
- d_out: bfloat16 [4096, 2048], P(('grp', 'ep')), may hold values from -12 to 12
- routes: int32 [4096, 2], P(('grp', 'ep')), may hold values from 0 to 7, all different within a row; in each aligned block of 128 rows (0 to 127, 128 to 255, ...) at most 48 rows name the same one
- combine: float32 [4096, 2], P(('grp', 'ep')), may hold values from 0.05 to 1
- live_tokens: int32 [32], P(('grp', 'ep')), may hold values from 1 to 128, as said below
- hidden: bfloat16 [1536, 57344], P('grp', 'ep'), may hold values from -6 to 6
Outputs:
- expert_grad: float32 [2048, 57344], P('grp', 'ep')
The draws below stay inside these ranges and needn't reach their ends.
Inputs may be any that keep to these rules, and one draw needn't show every extreme that they name: `routes`: the two experts of a token differ. Among the 128 rows of one device no expert is named by more than 48 rows, and on some devices one expert is named by exactly 48 rows. `live_tokens`: the live tokens of a device are its first ones; on the last device all 128 are live.
All inputs are finite; a program needn't handle non-finite values.
Results may differ from the reference program's by a relative error of at most 0.0029.
Values may be sent and summed in bfloat16 or wider, within the bound.
A program may use at most 128 MiB of HBM per device.

```python
import math
import jax
import jax.numpy as jnp
import numpy as np
from jax import lax

EXPERTS = 8
DW = 2048
H = 7168
TOK_DEV = 128
CAP = 48
SLOTS_E = 384
BLOCKS = 32
TOKENS = 4096
N_GRP = 4
N_EP = 8


def draw_live_tokens(key, part):
    index = jnp.arange(BLOCKS, dtype=jnp.int32)
    lowest = TOK_DEV // 4
    base = lowest + (TOK_DEV - lowest) * index // max(BLOCKS - 1, 1)
    jitter = jax.random.randint(jax.random.fold_in(key, 17), (BLOCKS,), 0, TOK_DEV // 8 + 1, dtype=jnp.int32)
    jitter = jnp.where(index == BLOCKS - 1, 0, jitter)
    return jnp.clip(base - jitter, 1, TOK_DEV).astype(jnp.int32)


def block_levels(key, extent, shards, low, top_value):
    def one(dim, blocks):
        draws = jax.random.uniform(jax.random.fold_in(jax.random.fold_in(key, 6), dim), (blocks,), jnp.float32, low / len(shards), top_value / len(shards))
        return jnp.repeat(jnp.exp(draws), extent[dim] // blocks).reshape((-1,) + (1,) * (len(extent) - dim - 1))

    factor_of = one(*shards[0])
    for cut in shards[1:]:
        factor_of = factor_of * one(*cut)
    return factor_of


def assign_block(key, own, number, rows, amount, top, most, skew):
    sequence = jax.random.permutation(key, amount)
    crowded, common = load_shares(amount, rows * top, most, skew, True), load_shares(amount, rows * top, most, skew, False)
    places = jnp.arange(amount)

    def named(sizes, offset_by):
        used = int((sizes > 0).sum())
        fixed = max(1, used // 4)
        moved = fixed + (places - fixed + offset_by * (used - fixed)) % max(1, amount - fixed)
        return jnp.zeros((amount,), jnp.int32).at[sequence[jnp.where(places < fixed, places, moved)]].set(jnp.asarray(sizes, jnp.int32))

    sizes = jnp.where(number % 4 == 0, named(crowded, number // 4), named(common, number - number // 4 - 1))
    mixed = jax.random.permutation(jax.random.fold_in(own, 3), amount)
    donor, taker = mixed[0:amount // 2 * 2:2], mixed[1:amount // 2 * 2:2]
    slack = jnp.minimum(sizes[donor] - 1, most - sizes[taker]) // 2
    slack = jnp.where((donor == sequence[0]) | (taker == sequence[0]) | (sizes[taker] == 0), 0, jnp.maximum(slack, 0))
    moved = jax.random.randint(jax.random.fold_in(own, 4), (amount // 2,), 0, 1 << 20) % (slack + 1)
    sizes = sizes.at[donor].add(-moved).at[taker].add(moved)
    items = jnp.searchsorted(jnp.cumsum(sizes), jnp.arange(rows * top), side="right").astype(jnp.int32)
    table = items.reshape(top, rows).T
    table = table[jax.random.permutation(jax.random.fold_in(own, 1), rows)]
    offset_by = jax.random.randint(jax.random.fold_in(own, 2), (rows, 1), 0, top)
    return jnp.take_along_axis(table, (jnp.arange(top)[None, :] + offset_by) % top, axis=1)


def load_shares(amount, total, bound, skew, full):
    portions = [(1 << 20) // math.isqrt(grade ** skew) + 1 for grade in range(1, amount + 1)]
    largest = bound if full else min(bound, max(-(-total // amount), total * portions[0] // sum(portions)))
    least = 1 if total - largest >= amount - 1 else 0
    given, spare = [largest] + [least] * (amount - 1), total - largest - least * (amount - 1)
    while spare > 0:
        movable = [i for i in range(1, amount) if given[i] < largest] or [i for i in range(1, amount) if given[i] < bound]
        whole, budget = sum([portions[i] for i in movable]), spare
        for i in movable:
            addition = min(bound - given[i], max(1, budget * portions[i] // whole), spare)
            given[i] = given[i] + addition
            spare = spare - addition
    return np.array(given)


def noise(own_key, extent, deviation, limit, shards=(), held_as=jnp.bfloat16):
    gain = block_levels(own_key, extent, shards, -0.22, 0.18) if shards else 1.0
    array = jax.random.normal(own_key, extent, jnp.float32) * deviation * gain
    return jnp.minimum(jnp.maximum(array, -limit), limit).astype(held_as)


def setup_inputs(seed: int = 0) -> dict:
    streams_of = jax.random.split(jax.random.key(seed), 6)
    d_out = noise(streams_of[0], (TOKENS, DW), 2.0, 12.0, ((0, 32),))
    routes_keys = jax.random.split(jax.random.fold_in(streams_of[1], 1), TOKENS // TOK_DEV)
    routes_turns = jax.random.permutation(jax.random.fold_in(streams_of[1], 3), TOKENS // TOK_DEV)
    routes = jax.vmap(lambda own, number: assign_block(jax.random.fold_in(streams_of[1], 2), own, number, TOK_DEV, EXPERTS, 2, CAP, 2))(routes_keys, routes_turns).reshape((TOKENS, 2))
    combine = jnp.clip(jnp.exp(math.log(1.0) - 2.9957323 * jax.random.uniform(streams_of[2], (TOKENS, 2), jnp.float32) ** block_levels(streams_of[2], (TOKENS, 2), ((0, 32),), -0.2, 0.2)), 0.05, 1.0)
    live_tokens = draw_live_tokens(jax.random.fold_in(streams_of[5], 71), 0)
    hidden = noise(streams_of[4], (N_GRP * SLOTS_E, EXPERTS * H), 1.0, 6.0, ((0, 4), (1, 8)))
    return dict(d_out=d_out, routes=routes, combine=combine, live_tokens=live_tokens, hidden=hidden)


def device_slots(d_rows, route_rows, weight_rows, live_count):
    tokens_here = d_rows.shape[0]
    alive = (jnp.arange(tokens_here, dtype=jnp.int32) < live_count).astype(jnp.float32)
    scaled = weight_rows * alive[:, None]
    weighted = (d_rows.astype(jnp.float32)[:, None, :] * scaled[:, :, None]).astype(jnp.bfloat16)
    weighted = weighted.reshape(tokens_here * route_rows.shape[1], d_rows.shape[1])
    flat = route_rows.reshape(-1).astype(jnp.int32)
    chosen = (flat[:, None] == jnp.arange(EXPERTS, dtype=jnp.int32)[None, :]).astype(jnp.int32)
    before = (jnp.cumsum(chosen, axis=0, dtype=jnp.int32) - chosen).astype(jnp.int32)
    position = lax.optimization_barrier(jnp.sum(before * chosen, axis=1, dtype=jnp.int32))
    slot_index = (flat * CAP + position).astype(jnp.int32)
    placing = (jnp.arange(EXPERTS * CAP, dtype=jnp.int32)[:, None] == slot_index[None, :]).astype(jnp.bfloat16)
    buffer = jnp.dot(placing, weighted, preferred_element_type=jnp.float32).astype(jnp.bfloat16)
    alive_pairs = jnp.repeat(alive, route_rows.shape[1])
    counts = lax.optimization_barrier(jnp.sum(chosen.astype(jnp.float32) * alive_pairs[:, None], axis=0))
    return (buffer.reshape(EXPERTS, CAP, d_rows.shape[1]), counts)

def reference(d_out, routes, combine, live_tokens, hidden):
    width = d_out.shape[1]
    group_tokens = N_EP * TOK_DEV

    def group_part(group):
        start = (group * group_tokens).astype(jnp.int32)
        rows = lax.dynamic_slice_in_dim(d_out, start, group_tokens, 0).reshape(N_EP, TOK_DEV, width)
        picks = lax.dynamic_slice_in_dim(routes, start, group_tokens, 0).reshape(N_EP, TOK_DEV, 2)
        weights = lax.dynamic_slice_in_dim(combine, start, group_tokens, 0).reshape(N_EP, TOK_DEV, 2)
        lives = lax.dynamic_slice_in_dim(live_tokens, (group * N_EP).astype(jnp.int32), N_EP, 0)
        buffers, counts = jax.vmap(device_slots)(rows, picks, weights, lives)

        def one_expert(expert):
            slots = lax.dynamic_index_in_dim(buffers, expert, 1, keepdims=False).reshape(N_EP * CAP, width)
            block = lax.dynamic_slice(hidden, ((group * SLOTS_E).astype(jnp.int32), (expert * H).astype(jnp.int32)), (SLOTS_E, H))
            return lax.dot_general(slots, block, (((0,), (0,)), ((), ())), preferred_element_type=jnp.float32)
        partial_value = lax.map(one_expert, jnp.arange(EXPERTS, dtype=jnp.int32))
        return (partial_value, lax.optimization_barrier(jnp.sum(counts, axis=0)))

    def step(carry, group):
        total, count = carry
        partial_value, counts = group_part(group)
        return ((total + partial_value, count + counts), None)
    start = (jnp.zeros((EXPERTS, width, H), jnp.float32), jnp.zeros((EXPERTS,), jnp.float32))
    (total, count), _ = lax.scan(step, start, jnp.arange(N_GRP, dtype=jnp.int32))
    result = total * lax.rsqrt(1.0 + count)[:, None, None]
    return jnp.transpose(result, (1, 0, 2)).reshape(width, EXPERTS * H)
```

```python
import functools

import jax
import jax.numpy as jnp
from jax import lax
from jax.experimental import pallas as pl
from jax.experimental.pallas import tpu as pltpu
from jax.sharding import PartitionSpec as P

EXPERTS = 8
CAP = 48
CORES = 2
EARLY = 16
LANES = 128
MESH = pl.DeviceIdType.MESH
MIB = 1024 * 1024


def pick_chunks(columns, wide):
    return columns // wide if columns % wide == 0 else columns // 256


def early_kernel(n_grp, n_ep, ladder, routes_in, combine_in, live, d_out, hidden, arrived, early, packed, targets, info,
                 routes, combine, held, mixed, cards, table, tokens_in, buffer, staged,
                 card_send, card_recv, tok_send, tok_recv, tab_send, tab_recv, slot_send, slot_recv,
                 far_send, far_recv, own_sem):
    n_y = n_grp // CORES
    grp, ep = lax.axis_index("grp"), lax.axis_index("ep")
    shards = n_ep // EXPERTS
    y, core = grp // CORES, lax.rem(grp, CORES)
    block = tokens_in.shape[2]
    slots, columns = hidden.shape
    tokens = routes.shape[1]
    first_rows = n_ep * EARLY
    barrier = pltpu.get_barrier_semaphore()

    def in_grp(j):
        return {"grp": lax.rem(grp + j, n_grp), "ep": ep}

    def in_ep(j):
        return {"grp": grp, "ep": lax.rem(ep + j, n_ep)}

    def loop(low, high, body):
        def step(j, _):
            body(j)
            return 0

        lax.fori_loop(low, high, step, 0)

    loop(1, n_grp, lambda j: pl.semaphore_signal(barrier, inc=1, device_id=in_grp(j), device_id_type=MESH))
    loop(1, n_ep, lambda j: pl.semaphore_signal(barrier, inc=1, device_id=in_ep(j), device_id_type=MESH))

    router_copies = [
        pltpu.make_async_copy(routes_in, routes, own_sem.at[2]), pltpu.make_async_copy(combine_in, combine, own_sem.at[3])]
    for copy in router_copies:
        copy.start()
    held_copy = pltpu.make_async_copy(hidden, held, own_sem.at[0])
    held_copy.start()

    def token_block(i):
        return d_out.at[:, pl.ds(pl.multiple_of(i * block, LANES), block)]

    tokens_mine = pltpu.make_async_copy(token_block(grp), tokens_in.at[grp], own_sem.at[1])
    tokens_mine.start()

    for copy in router_copies:
        copy.wait()
    alive = jnp.where(lax.broadcasted_iota(jnp.int32, (1, tokens), 1) < live[0], 1.0, 0.0)
    cards[grp, 0:2, :] = routes[...].astype(jnp.float32)
    cards[grp, 2:4, :] = combine[...] * alive
    cards[grp, 4:8, :] = jnp.broadcast_to(alive, (4, tokens))
    pl.semaphore_wait(barrier, n_grp - 1 + n_ep - 1)

    def card_copy(j, owner):
        return pltpu.make_async_remote_copy(
            src_ref=cards.at[owner], dst_ref=cards.at[owner], send_sem=card_send.at[j], recv_sem=card_recv.at[j],
            device_id=in_grp(j), device_id_type=MESH)

    def token_copy(j):
        return pltpu.make_async_remote_copy(
            src_ref=token_block(lax.rem(grp + j, n_grp)), dst_ref=tokens_in.at[grp],
            send_sem=tok_send.at[j], recv_sem=tok_recv.at[j], device_id=in_grp(j), device_id_type=MESH)

    def token_arrival(j):
        here = tokens_in.at[lax.rem(grp - j + n_grp, n_grp)]
        return pltpu.make_async_remote_copy(
            src_ref=here, dst_ref=here, send_sem=tok_send.at[j], recv_sem=tok_recv.at[j],
            device_id=in_grp(j), device_id_type=MESH)

    loop(1, n_grp, lambda j: card_copy(j, grp).start())
    loop(1, n_grp, lambda j: token_copy(j).start())

    def far_copy(j, s, owner):
        return pltpu.make_async_remote_copy(
            src_ref=hidden.at[pl.ds(pl.multiple_of(s * CAP, 16), EARLY), :],
            dst_ref=early.at[owner, pl.ds(pl.multiple_of(s * EARLY, 16), EARLY), :],
            send_sem=far_send.at[j, s], recv_sem=far_recv.at[j, s],
            device_id={"grp": lax.rem(y + j, n_y) * CORES + core, "ep": ep}, device_id_type=MESH)

    for j in range(1, n_y):
        loop(0, n_ep, lambda s: far_copy(j, s, grp).start())

    loop(1, n_grp, lambda j: card_copy(j, lax.rem(grp - j + n_grp, n_grp)).wait_recv())

    expert_rows = lax.broadcasted_iota(jnp.int32, (LANES, tokens), 0).astype(jnp.float32)

    def count_group(g):
        card = cards[g]
        chosen = jnp.where(expert_rows == card[0:1, :], 1.0, 0.0) + jnp.where(expert_rows == card[1:2, :], 1.0, 0.0)
        lives = jnp.broadcast_to(card[4:5, :], (8, tokens))
        table[ep, g] = lax.dot_general(
            lives.astype(jnp.bfloat16), chosen.astype(jnp.bfloat16), (((1,), (1,)), ((), ())),
            preferred_element_type=jnp.float32)

    loop(0, n_grp, count_group)

    def table_copy(j, owner):
        return pltpu.make_async_remote_copy(
            src_ref=table.at[owner], dst_ref=table.at[owner], send_sem=tab_send.at[j], recv_sem=tab_recv.at[j],
            device_id=in_ep(j), device_id_type=MESH)

    loop(1, n_ep, lambda j: table_copy(j, ep).start())

    square = (tokens, tokens)
    earlier = jnp.where(
        lax.broadcasted_iota(jnp.int32, square, 0) < lax.broadcasted_iota(jnp.int32, square, 1), 1.0, 0.0
    ).astype(jnp.bfloat16)
    slot_rows = lax.broadcasted_iota(jnp.int32, (EXPERTS * CAP, tokens), 0).astype(jnp.float32)

    def fill_group(g):
        card = cards[g]
        picks = [card[k : k + 1, :] for k in range(2)]
        chosen = [jnp.where(expert_rows[0:16, :] == pick, 1.0, 0.0) for pick in picks]
        running = jnp.dot(sum(chosen).astype(jnp.bfloat16), earlier, preferred_element_type=jnp.float32)
        tall = jnp.concatenate([card] * (tokens // 8), axis=0).T
        rows = tokens_in[g].astype(jnp.float32)
        total = None
        for k in range(2):
            position = jnp.sum(chosen[k] * running, axis=0, keepdims=True)
            running = running + chosen[k]
            put = jnp.where(slot_rows == picks[k] * CAP + position, 1.0, 0.0).astype(jnp.bfloat16)
            weighted = (rows * tall[:, 2 + k : 3 + k]).astype(jnp.bfloat16)
            term = jnp.dot(put, weighted, preferred_element_type=jnp.float32)
            total = term if total is None else total + term
        buffer[g] = total.astype(buffer.dtype)

    tokens_mine.wait()
    loop(1, n_grp, lambda j: token_arrival(j).wait_recv())
    loop(0, n_grp, fill_group)

    def expert_slots(expert):
        return buffer.at[:, pl.ds(pl.multiple_of(expert * CAP, CAP), CAP), :]

    def slot_place(source):
        return arrived.at[:, pl.ds(pl.multiple_of(source * CAP, CAP), CAP), :]

    def slot_copy(j):
        target = lax.rem(ep + j, n_ep)
        return pltpu.make_async_remote_copy(
            src_ref=expert_slots(target // shards), dst_ref=slot_place(ep),
            send_sem=slot_send.at[j], recv_sem=slot_recv.at[j],
            device_id={"grp": grp, "ep": target}, device_id_type=MESH)

    def slot_arrival(j):
        here = slot_place(lax.rem(ep - j + n_ep, n_ep))
        return pltpu.make_async_remote_copy(
            src_ref=here, dst_ref=here, send_sem=slot_send.at[j], recv_sem=slot_recv.at[j],
            device_id=in_ep(j), device_id_type=MESH)

    loop(1, n_ep, lambda j: slot_copy(j).start())
    slots_mine = pltpu.make_async_copy(expert_slots(ep // shards), slot_place(ep), own_sem.at[1])
    slots_mine.start()
    loop(1, n_ep, lambda j: table_copy(j, lax.rem(ep - j + n_ep, n_ep)).wait_recv())

    mine = lax.broadcasted_iota(jnp.int32, (8, LANES), 1) == ep // shards
    slot = lax.broadcasted_iota(jnp.int32, (8, slots), 1)
    source = slot // CAP
    place = (slot - source * CAP).astype(jnp.float32)

    def target_group(g):
        def one(s, state):
            filled, first, before = state
            amount = jnp.sum(jnp.where(mine, table[s, g], 0.0), axis=1, keepdims=True)
            here = source == s
            filled = filled + jnp.where(here, amount, 0.0)
            first = first + jnp.where(here, before, 0.0)
            return filled, first, before + jnp.maximum(amount - EARLY, 0.0)

        nothing = jnp.zeros((8, slots), jnp.float32)
        state = (nothing, nothing, jnp.zeros((8, 1), jnp.float32))
        for s in range(n_ep):
            state = one(s, state)
        filled, first, _ = state
        staged[g] = jnp.where((place < filled) & (place >= EARLY), first + place - EARLY, -1.0)

    loop(0, n_grp, target_group)
    target = staged[grp, 0:1, :]
    rows = 64 if mixed.shape[0] % 64 == 0 else mixed.shape[0]

    def write(i):
        start = pl.multiple_of(i * rows, rows)
        index = (lax.broadcasted_iota(jnp.int32, (rows, slots), 0) + start).astype(jnp.float32)
        mixed[pl.ds(start, rows), 0:slots] = jnp.where(index == target, 1.0, 0.0).astype(mixed.dtype)

    loop(0, mixed.shape[0] // rows, write)
    held_copy.wait()
    chunks = pick_chunks(columns, 512)
    wide = columns // chunks

    def packed_copy(i):
        part = pl.ds(pl.multiple_of(i * wide, LANES), wide)
        return pltpu.make_async_copy(mixed.at[:, pl.ds(pl.multiple_of(slots + i * wide, LANES), wide)], packed.at[:, part], own_sem.at[2 + i])

    def pack(i):
        part = pl.ds(pl.multiple_of(i * wide, LANES), wide)
        mixed[:, pl.ds(pl.multiple_of(slots + i * wide, LANES), wide)] = jnp.dot(
            mixed[:, 0:slots], held[:, part], preferred_element_type=jnp.float32).astype(packed.dtype)

        @pl.when(i > 0)
        def _():
            packed_copy(i - 1).start()

    loop(0, chunks, pack)

    need = [jnp.zeros((8, LANES), jnp.float32) for _ in range(CORES)]
    count = jnp.zeros((8, LANES), jnp.float32)
    for g in range(n_grp):
        kept = jnp.zeros((8, LANES), jnp.float32)
        for s in range(n_ep):
            kept = kept + jnp.maximum(table[s, g] - EARLY, 0.0)
            count = count + table[s, g]
        need[g % CORES] = jnp.maximum(need[g % CORES], kept)
    count = jnp.sum(jnp.where(mine, count, 0.0), axis=1, keepdims=True)
    need = [jnp.max(n, axis=1, keepdims=True) for n in need]
    branch = jnp.zeros((8, 1), jnp.float32)
    for keep in ladder:
        branch = branch + jnp.where((need[0] <= keep[0]) & (need[1] <= keep[1]), 0.0, 1.0)
    info[0:8, :] = jnp.broadcast_to(count, (8, LANES))
    info[8:16, :] = jnp.broadcast_to(branch, (8, LANES))
    packed_copy(chunks - 1).start()
    targets[...] = staged[...]

    def early_copy(s):
        return pltpu.make_async_copy(
            held.at[pl.ds(pl.multiple_of(s * CAP, 16), EARLY), :],
            early.at[grp, pl.ds(pl.multiple_of(s * EARLY, 16), EARLY), :], own_sem.at[2 + chunks + s])

    loop(0, n_ep, lambda s: early_copy(s).start())
    loop(0, n_ep, lambda s: early_copy(s).wait())
    loop(0, chunks, lambda i: packed_copy(i).wait())
    slots_mine.wait()

    def leave_grp(j):
        card_copy(j, grp).wait_send()
        token_copy(j).wait_send()

    def leave_ep(j):
        table_copy(j, ep).wait_send()
        slot_copy(j).wait_send()
        slot_arrival(j).wait_recv()

    loop(1, n_grp, leave_grp)
    loop(1, n_ep, leave_ep)
    for j in range(1, n_y):
        peer = lax.rem(y - j + n_y, n_y) * CORES + core

        def leave_far(s):
            far_copy(j, s, grp).wait_send()
            far_copy(j, s, peer).wait_recv()

        loop(0, n_ep, leave_far)


def in_hbm(array):
    return pltpu.with_memory_space_constraint(array, pltpu.HBM)


def gather_early(routes, combine, live, d_out, hidden, ladder, n_grp, n_ep):
    n_y = n_grp // CORES
    slots, columns = hidden.shape
    tokens, width = d_out.shape
    block = width // n_grp
    rest = n_ep * (CAP - EARLY)
    chunks = pick_chunks(columns, 512)
    dma = pltpu.SemaphoreType.DMA
    vmem, smem, hbm = (pl.BlockSpec(memory_space=m) for m in (pltpu.VMEM, pltpu.SMEM, pltpu.HBM))
    return pl.pallas_call(
        functools.partial(early_kernel, n_grp, n_ep, ladder),
        out_shape=(
            jax.ShapeDtypeStruct((n_grp, slots, block), d_out.dtype),
            jax.ShapeDtypeStruct((n_grp, n_ep * EARLY, columns), hidden.dtype),
            jax.ShapeDtypeStruct((rest, columns), hidden.dtype),
            jax.ShapeDtypeStruct((n_grp, 8, slots), jnp.float32),
            jax.ShapeDtypeStruct((16, LANES), jnp.float32),
        ),
        in_specs=[hbm, hbm, smem, hbm, hbm],
        out_specs=(hbm, hbm, hbm, vmem, vmem),
        scratch_shapes=[
            pltpu.VMEM((2, tokens), routes.dtype),
            pltpu.VMEM((2, tokens), combine.dtype),
            pltpu.VMEM((slots, columns), hidden.dtype),
            pltpu.VMEM((rest, slots + columns), hidden.dtype),
            pltpu.VMEM((n_grp, 8, tokens), jnp.float32),
            pltpu.VMEM((n_ep, n_grp, 8, LANES), jnp.float32),
            pltpu.VMEM((n_grp, tokens, block), d_out.dtype),
            pltpu.VMEM((n_grp, EXPERTS * CAP, block), d_out.dtype),
            pltpu.VMEM((n_grp, 8, slots), jnp.float32),
            dma((n_grp,)), dma((n_grp,)), dma((n_grp,)), dma((n_grp,)),
            dma((n_ep,)), dma((n_ep,)), dma((n_ep,)), dma((n_ep,)),
            dma((n_y, n_ep)), dma((n_y, n_ep)),
            dma((2 + chunks + n_ep,)),
        ],
        compiler_params=pltpu.CompilerParams(collective_id=0, has_side_effects=True, vmem_limit_bytes=40 * MIB),
        name="gather_early",
    )(in_hbm(routes), in_hbm(combine), live, in_hbm(d_out), in_hbm(hidden))


def rest_kernel(n_grp, n_ep, keep, arrived, early, packed, targets, info, out, whole, turned, slots_in,
                far_send, far_recv, relay_send, relay_recv, near_send, near_recv, first_send, first_recv, own_sem):
    n_y = n_grp // CORES
    grp, ep = lax.axis_index("grp"), lax.axis_index("ep")
    y, core = grp // CORES, lax.rem(grp, CORES)
    pair = keep[0] + keep[1]
    first_rows = early.shape[1]
    base = n_grp * first_rows
    used = base + n_y * pair
    depth = whole.shape[0]
    columns = packed.shape[1]
    slots = arrived.shape[1]
    block = arrived.shape[2]
    chunks = pick_chunks(columns, 512)
    wide = columns // chunks
    barrier = pltpu.get_barrier_semaphore()

    def loop(low, high, body):
        def step(j, _):
            body(j)
            return 0

        lax.fori_loop(low, high, step, 0)

    def mate(which):
        return {"grp": y * CORES + (1 - which), "ep": ep}

    def at_y(j, which):
        return {"grp": lax.rem(y + j, n_y) * CORES + which, "ep": ep}

    def each_core(body):
        for which in range(CORES):
            pl.when(core == which)(functools.partial(body, which))

    def greet(which):
        for j in range(1, n_y):
            pl.semaphore_signal(barrier, inc=1, device_id=at_y(j, which), device_id_type=MESH)
        pl.semaphore_signal(barrier, inc=1, device_id=mate(which), device_id_type=MESH)

    each_core(greet)

    def part(i):
        return pl.ds(pl.multiple_of(i * wide, LANES), wide)

    def span(row, which):
        start = base + row * pair + (0 if which == 0 else keep[0])
        return pl.ds(pl.multiple_of(start, 16), keep[which])

    def first_span(g):
        return pl.ds(pl.multiple_of(g * first_rows, 16), first_rows)

    def far_copy(which, j, i, row):
        return pltpu.make_async_remote_copy(
            src_ref=packed.at[pl.ds(0, keep[which]), part(i)], dst_ref=whole.at[span(row, which), part(i)],
            send_sem=far_send.at[j, i], recv_sem=far_recv.at[j, i], device_id=at_y(j, which), device_id_type=MESH)

    def relay_copy(which, j, i, cell):
        here = whole.at[span(lax.rem(y - j + n_y, n_y), cell), part(i)]
        return pltpu.make_async_remote_copy(
            src_ref=here, dst_ref=here, send_sem=relay_send.at[j, i], recv_sem=relay_recv.at[j, i],
            device_id=mate(which), device_id_type=MESH)

    def near_copy(which):
        return pltpu.make_async_remote_copy(
            src_ref=packed.at[pl.ds(0, keep[which]), :], dst_ref=whole.at[span(y, which), :],
            send_sem=near_send, recv_sem=near_recv, device_id=mate(which), device_id_type=MESH)

    def near_arrival(which):
        here = whole.at[span(y, 1 - which), :]
        return pltpu.make_async_remote_copy(
            src_ref=here, dst_ref=here, send_sem=near_send, recv_sem=near_recv,
            device_id=mate(which), device_id_type=MESH)

    def first_copy(which, row):
        g = row * CORES + which
        return pltpu.make_async_remote_copy(
            src_ref=early.at[g], dst_ref=whole.at[first_span(g), :],
            send_sem=first_send.at[row], recv_sem=first_recv.at[row], device_id=mate(which), device_id_type=MESH)

    def first_arrival(which, row):
        here = whole.at[first_span(row * CORES + (1 - which)), :]
        return pltpu.make_async_remote_copy(
            src_ref=here, dst_ref=here, send_sem=first_send.at[row], recv_sem=first_recv.at[row],
            device_id=mate(which), device_id_type=MESH)

    def own_copy(which):
        return pltpu.make_async_copy(packed.at[pl.ds(0, keep[which]), :], whole.at[span(y, which), :], own_sem.at[0])

    def own_first(which, row):
        g = row * CORES + which
        return pltpu.make_async_copy(early.at[g], whole.at[first_span(g), :], own_sem.at[1 + row])

    def slots_copy(g):
        return pltpu.make_async_copy(arrived.at[g], slots_in.at[g], own_sem.at[1 + n_y + g])

    pl.semaphore_wait(barrier, n_y)

    def begin(which):
        for j in range(1, n_y):
            loop(0, chunks, lambda i: far_copy(which, j, i, y).start())
        near_copy(which).start()
        loop(0, n_y, lambda row: first_copy(which, row).start())

    each_core(begin)
    loop(0, n_grp, lambda g: slots_copy(g).start())

    def begin_own(which):
        own_copy(which).start()
        loop(0, n_y, lambda row: own_first(which, row).start())

    each_core(begin_own)
    if depth > used:
        whole[used:depth, :] = jnp.zeros((depth - used, columns), whole.dtype)
    loop(0, n_grp, lambda g: slots_copy(g).wait())

    per = LANES // EARLY

    def turn_first(i):
        g = i // (first_rows // LANES)
        s = lax.rem(i, first_rows // LANES) * per
        rows = jnp.concatenate(
            [slots_in[g, pl.ds(pl.multiple_of((s + k) * CAP, 16), EARLY), :] for k in range(per)], axis=0)
        turned[:, pl.ds(pl.multiple_of(i * LANES, LANES), LANES)] = rows.astype(jnp.float32).T.astype(turned.dtype)

    loop(0, base // LANES, turn_first)

    def turn_rest(start, groups):
        rows = jnp.zeros((LANES, block), jnp.float32)
        for g, low in groups:
            index = (lax.broadcasted_iota(jnp.int32, (LANES, slots), 0) + (start - low)).astype(jnp.float32)
            pick = jnp.where(index == targets[g, 0:1, :], 1.0, 0.0).astype(jnp.bfloat16)
            rows = rows + jnp.dot(pick, slots_in[g], preferred_element_type=jnp.float32)
        turned[:, start : start + LANES] = rows.T.astype(turned.dtype)

    lows = [base + (g // CORES) * pair + (g % CORES) * keep[0] for g in range(n_grp)]
    for start in range(base, depth, LANES):
        turn_rest(start, [
            (g, low) for g, low in enumerate(lows) if low < start + LANES and low + keep[g % CORES] > start])

    def settle(which):
        own_copy(which).wait()
        near_arrival(which).wait_recv()

        def row_done(row):
            own_first(which, row).wait()
            first_arrival(which, row).wait_recv()

        loop(0, n_y, row_done)

    each_core(settle)
    scale = lax.rsqrt(1.0 + info[0:1, 0:1])

    def step(i):
        def take(which):
            for j in range(1, n_y):
                far_copy(which, j, i, lax.rem(y - j + n_y, n_y)).wait_recv()
                relay_copy(which, j, i, which).start()
            for j in range(1, n_y):
                relay_copy(which, j, i, 1 - which).wait_recv()

        each_core(take)
        out[:, part(i)] = scale * jnp.dot(turned[...], whole[:, part(i)], preferred_element_type=jnp.float32)

    loop(0, chunks, step)

    def finish(which):
        near_copy(which).wait_send()
        loop(0, n_y, lambda row: first_copy(which, row).wait_send())
        for j in range(1, n_y):
            def leave(i):
                far_copy(which, j, i, y).wait_send()
                relay_copy(which, j, i, which).wait_send()

            loop(0, chunks, leave)

    each_core(finish)


def multiply_rest(number, keep, arrived, early, packed, targets, info, n_grp, n_ep):
    n_y = n_grp // CORES
    _, slots, block = arrived.shape
    columns = packed.shape[1]
    used = n_grp * early.shape[1] + n_y * (keep[0] + keep[1])
    depth = -(-used // LANES) * LANES
    chunks = pick_chunks(columns, 512)
    dma = pltpu.SemaphoreType.DMA
    vmem, hbm = (pl.BlockSpec(memory_space=m) for m in (pltpu.VMEM, pltpu.HBM))
    room = 2 * (depth * (columns + block) + n_grp * slots * block) + 6 * MIB
    return pl.pallas_call(
        functools.partial(rest_kernel, n_grp, n_ep, keep),
        out_shape=pltpu.VMEM((block, columns), jnp.float32),
        in_specs=[hbm, hbm, hbm, vmem, vmem],
        out_specs=vmem,
        scratch_shapes=[
            pltpu.VMEM((depth, columns), packed.dtype),
            pltpu.VMEM((block, depth), arrived.dtype),
            pltpu.VMEM((n_grp, slots, block), arrived.dtype),
            dma((n_y, chunks)), dma((n_y, chunks)), dma((n_y, chunks)), dma((n_y, chunks)),
            dma, dma, dma((n_y,)), dma((n_y,)),
            dma((1 + n_y + n_grp,)),
        ],
        compiler_params=pltpu.CompilerParams(
            collective_id=1 + number, has_side_effects=True, vmem_limit_bytes=room),
        name=f"multiply_rest_{number}",
    )(arrived, early, packed, targets, info)


def store_kernel(total, out, sems):
    parts = sems.shape[0]
    rows = total.shape[0] // parts
    copies = [
        pltpu.make_async_copy(total.at[i * rows : (i + 1) * rows], out.at[i * rows : (i + 1) * rows], sems.at[i])
        for i in range(parts)]
    for copy in copies:
        copy.start()
    for copy in copies:
        copy.wait()


def store(total):
    return pl.pallas_call(
        store_kernel,
        out_shape=pltpu.HBM(total.shape, total.dtype),
        in_specs=[pl.BlockSpec(memory_space=pltpu.VMEM)],
        out_specs=pl.BlockSpec(memory_space=pltpu.HBM),
        scratch_shapes=[pltpu.SemaphoreType.DMA((8,))],
        compiler_params=pltpu.CompilerParams(vmem_limit_bytes=MIB),
        name="store",
    )(total)


def on_device(d_out, routes, combine, live_tokens, hidden):
    n_grp, n_ep = lax.axis_size("grp"), lax.axis_size("ep")
    rest = n_ep * (CAP - EARLY)
    step = rest // 16
    sizes = ((9 * step, 13 * step), (9 * step, 14 * step), (16 * step, 16 * step))
    arrived, early, packed, targets, info = gather_early(
        routes.T, combine.T, live_tokens, d_out, hidden, sizes[:-1], n_grp, n_ep)
    branch = info[8, 0].astype(jnp.int32)

    def run(number, *operands):
        return store(multiply_rest(number, sizes[number], *operands, n_grp, n_ep))

    branches = [functools.partial(run, n) for n in range(len(sizes))]
    return lax.switch(branch, branches, arrived, early, packed, targets, info)


def solution(mesh):
    return jax.shard_map(
        on_device,
        mesh=mesh,
        in_specs=(
            P(("grp", "ep"), None),
            P(("grp", "ep"), None),
            P(("grp", "ep"), None),
            P(("grp", "ep")),
            P("grp", "ep"),
        ),
        out_specs=P("grp", "ep"),
        check_vma=False,
    )
```
